32 devices in a mesh: ov: 16 (over z, y, core), vec: 2 (over x).
Axes of the slice: x: 2, y: 2, z: 4, core: 2. Of those that a mesh axis runs over, the one named last changes fastest.
Arguments:
- chol_vectors: bfloat16 [196608, 4096], P('ov', 'vec'), may hold values from -3.5 to 3.5
- amplitudes: bfloat16 [196608, 256], P('ov'), may hold values from -0.013671875 to 0.013671875
- sigma_prior: bfloat16 [196608, 256], P(('ov', 'vec')), may hold values from -4 to 4
Outputs:
- sigma_cycle: bfloat16 [196608, 256], P(('ov', 'vec'))
The draws below stay inside these ranges and needn't reach their ends.
All inputs are finite; a program needn't handle non-finite values.
Results may differ from the reference program's by a relative error of at most 0.0065.
Values may be sent and summed in bfloat16 or wider, within the bound.
A program may use at most 128 MiB of HBM per device.

```python
import jax
import jax.numpy as jnp
from jax import lax

OV = 196608
NV = 4096
JB = 256


def with_spikes(values, key, source, target, parts, factor):
    def block_of(dim):
        return (jnp.arange(values.shape[dim]) // (values.shape[dim] // parts)).reshape((-1,) + (1,) * (values.ndim - 1 - dim))

    one_side = jax.random.permutation(key, parts)[block_of(target)]
    second = (block_of(target) + parts // 2) % parts
    return jnp.where((block_of(source) == one_side) | (block_of(source) == second), factor * values, values)


def steps_of(key, dims, cuts, low, high):
    gain, own = 1.0, jax.random.fold_in(key, 6)
    for axis_at, blocks in cuts:
        draws = jnp.exp(jax.random.uniform(jax.random.fold_in(own, axis_at), (blocks,), jnp.float32, low / len(cuts), high / len(cuts)))
        gain = gain * jnp.repeat(draws, dims[axis_at] // blocks).reshape([-1 if axis == axis_at else 1 for axis in range(len(dims))])
    return gain


def bell_draw(own_key, shape, deviation, bound, pieces=(), held_as=jnp.bfloat16):
    gain = steps_of(own_key, shape, pieces, -0.22, 0.18) if pieces else 1.0
    result = jax.random.normal(own_key, shape, jnp.float32) * deviation * gain
    return jnp.minimum(jnp.maximum(result, -bound), bound).astype(held_as)


def gaussian_with(rng, extent, width, reach, cuts, heavy, dtype=jnp.bfloat16):
    values = width * jax.random.normal(rng, extent, jnp.float32)
    if cuts:
        values = values * steps_of(rng, extent, cuts, -0.22, 0.18)
    return jnp.clip(with_spikes(values, jax.random.fold_in(rng, 3), *heavy), -reach, reach).astype(dtype)


def setup_inputs(seed: int = 0) -> dict:
    splits = jax.random.split(jax.random.key(seed), 4)
    chol_vectors = gaussian_with(splits[0], (OV, NV), 0.177, 3.5, ((0, 16), (1, 2)), (1, 0, 16, 2.0))
    amplitudes = bell_draw(splits[1], (OV, JB), OV ** -0.5, 0.013671875, ((0, 16),))
    sigma_prior = bell_draw(splits[2], (OV, JB), 0.5, 4.0, ((0, 32),))
    return {"chol_vectors": chol_vectors, "amplitudes": amplitudes, "sigma_prior": sigma_prior}


def reference(chol_vectors, amplitudes, sigma_prior):
    contract = (((0,), (0,)), ((), ()))
    coupling = lax.dot_general(chol_vectors, amplitudes, contract, preferred_element_type=jnp.float32)
    coupling_bf = coupling.astype(jnp.bfloat16)
    cycle = jnp.dot(chol_vectors, coupling_bf, preferred_element_type=jnp.float32)
    return (sigma_prior.astype(jnp.float32) + cycle).astype(jnp.bfloat16)
```

```python
import functools

import jax
import jax.numpy as jnp
from jax import lax
from jax.experimental import pallas as pl
from jax.experimental.pallas import tpu as pltpu
from jax.sharding import PartitionSpec as P

COLUMN_CHUNKS = 1
MESH = pl.DeviceIdType.MESH
ROW_CHUNKS = 6


def share_kernel(start, chol, coupling, out):
    out[...] = jnp.dot(
        chol[...], coupling[...], preferred_element_type=jnp.float32
    ).astype(out.dtype)


def final_kernel(received, start, chol, coupling, prior, *rest):
    out = rest[-1]
    total = jnp.dot(chol[...], coupling[...], preferred_element_type=jnp.float32)
    for share in rest[:received]:
        total += share[...].astype(jnp.float32)
    out[...] = (prior[...].astype(jnp.float32) + total).astype(out.dtype)


def tile_of(rows):
    tile = 512
    while rows % tile:
        tile //= 2
    return tile


def cost(rows, depth, width):
    return pl.CostEstimate(
        flops=2 * rows * depth * width,
        bytes_accessed=2 * (rows * depth + depth * width + rows * width),
        transcendentals=0,
    )


def share(chol, coupling, start, rows):
    depth, width = coupling.shape
    tile = tile_of(rows)
    return pl.pallas_call(
        share_kernel,
        out_shape=jax.ShapeDtypeStruct((rows, width), jnp.bfloat16),
        grid_spec=pltpu.PrefetchScalarGridSpec(
            num_scalar_prefetch=1,
            grid=(rows // tile,),
            in_specs=[
                pl.BlockSpec((tile, depth), lambda i, s: (s[0] // tile + i, 0)),
                pl.BlockSpec((depth, width), lambda i, s: (0, 0)),
            ],
            out_specs=pl.BlockSpec((tile, width), lambda i, s: (i, 0)),
        ),
        cost_estimate=cost(rows, depth, width),
    )(start.reshape(1), chol, coupling)


def finish(chol, coupling, start, prior, shares, row_at, column_at, out):
    depth, width = coupling.shape
    rows = shares[0].shape[0]
    tile = tile_of(rows)
    place = lambda i, s: (row_at // tile + i, column_at // width)
    inputs = [start.reshape(1), chol, coupling, prior, *shares]
    specs = [
        pl.BlockSpec((tile, depth), lambda i, s: ((s[0] + row_at) // tile + i, 0)),
        pl.BlockSpec((depth, width), lambda i, s: (0, 0)),
        pl.BlockSpec((tile, width), place),
    ] + [pl.BlockSpec((tile, width), lambda i, s: (i, 0)) for _ in shares]
    aliases = {}
    if out is not None:
        aliases = {len(inputs): 0}
        inputs.append(out)
        specs.append(pl.BlockSpec(memory_space=pl.ANY))
    return pl.pallas_call(
        functools.partial(final_kernel, len(shares)),
        out_shape=jax.ShapeDtypeStruct(prior.shape, prior.dtype),
        grid_spec=pltpu.PrefetchScalarGridSpec(
            num_scalar_prefetch=1,
            grid=(rows // tile,),
            in_specs=specs,
            out_specs=pl.BlockSpec((tile, width), place),
        ),
        input_output_aliases=aliases,
        cost_estimate=cost(rows, depth, width),
    )(*inputs)


def sum_kernel(n, partial, out, paired, halves, arrived, pair_sems, send_sems, recv_sems, give_sems, take_sems, on_sems, last_sems):
    half = n // 2
    me = lax.axis_index("ov")
    side = lax.rem(me, 2)
    group = me // 2
    twin = me + 1 - 2 * side

    def there(device):
        return {"ov": device}

    def mate(step):
        return 2 * lax.rem(group + step, half) + side

    def origin(step):
        return lax.rem(group + half - step, half)

    barrier = pltpu.get_barrier_semaphore()
    pl.semaphore_signal(barrier, inc=1, device_id=there(twin), device_id_type=MESH)

    @pl.loop(1, half)
    def _(step):
        pl.semaphore_signal(barrier, inc=1, device_id=there(mate(step)), device_id_type=MESH)

    pl.semaphore_wait(barrier, half)

    swap = pltpu.make_async_remote_copy(
        src_ref=partial.at[1 - side],
        dst_ref=paired,
        send_sem=pair_sems.at[0],
        recv_sem=pair_sems.at[1],
        device_id=there(twin),
        device_id_type=MESH,
    )
    swap.start()
    swap.wait()

    def scatter(step):
        return pltpu.make_async_remote_copy(
            src_ref=halves.at[lax.rem(group + step, half)],
            dst_ref=arrived.at[step],
            send_sem=send_sems.at[step],
            recv_sem=recv_sems.at[step],
            device_id=there(mate(step)),
            device_id_type=MESH,
        )

    @pl.loop(1, half)
    def _(step):
        at = lax.rem(group + step, half)
        halves[at] = (partial[side, at] + paired[at]).astype(halves.dtype)
        scatter(step).start()

    paired[group] = partial[side, group] + paired[group]

    @pl.loop(1, half)
    def _(step):
        scatter(step).wait()
        paired[group] += arrived[step].astype(jnp.float32)

    out[side, group] = paired[group].astype(out.dtype)

    def gather(step, slot):
        return pltpu.make_async_remote_copy(
            src_ref=out.at[side, slot],
            dst_ref=out.at[side, slot],
            send_sem=give_sems.at[step],
            recv_sem=take_sems.at[step],
            device_id=there(mate(step)),
            device_id_type=MESH,
        )

    def onward(step, hand):
        return pltpu.make_async_remote_copy(
            src_ref=out.at[hand, origin(step)],
            dst_ref=out.at[hand, origin(step)],
            send_sem=on_sems.at[step],
            recv_sem=last_sems.at[step],
            device_id=there(twin),
            device_id_type=MESH,
        )

    @pl.loop(1, half)
    def _(step):
        gather(step, group).start()

    onward(0, side).start()

    @pl.loop(1, half)
    def _(step):
        gather(step, origin(step)).wait_recv()
        onward(step, side).start()

    @pl.loop(1, half)
    def _(step):
        gather(step, group).wait_send()

    @pl.loop(0, half)
    def _(step):
        onward(step, side).wait_send()
        onward(step, 1 - side).wait_recv()


def all_sum(partial, n):
    depth, width = partial.shape
    half, piece = n // 2, depth // n
    summed = pl.pallas_call(
        functools.partial(sum_kernel, n),
        out_shape=jax.ShapeDtypeStruct((2, half, piece, width), jnp.bfloat16),
        in_specs=[pl.BlockSpec(memory_space=pltpu.VMEM)],
        out_specs=pl.BlockSpec(memory_space=pltpu.VMEM),
        scratch_shapes=[
            pltpu.VMEM((half, piece, width), jnp.float32),
            pltpu.VMEM((half, piece, width), jnp.bfloat16),
            pltpu.VMEM((half, piece, width), jnp.bfloat16),
            pltpu.SemaphoreType.DMA((2,)),
        ]
        + [pltpu.SemaphoreType.DMA((half,))] * 6,
        compiler_params=pltpu.CompilerParams(collective_id=0, has_side_effects=True),
    )(partial.reshape(2, half, piece, width))
    return summed.reshape(depth, width)


def body(n, groups, chol, amplitudes, prior):
    me = lax.axis_index("vec")
    rows, columns = prior.shape
    width = columns // COLUMN_CHUNKS
    piece = rows // ROW_CHUNKS
    contract = (((0,), (0,)), ((), ()))
    partial = lax.dot_general(
        chol, amplitudes, contract, preferred_element_type=jnp.float32
    )
    work = []
    for j in range(COLUMN_CHUNKS):
        coupling = all_sum(partial[:, j * width : (j + 1) * width], n)
        for k in range(ROW_CHUNKS):
            shares = []
            for d in range(1, groups):
                target = lax.rem(me + d, groups)
                mine = share(chol, coupling, target * rows + k * piece, piece)
                ring = [(g, (g + d) % groups) for g in range(groups)]
                shares.append(lax.ppermute(mine, "vec", ring))
            work.append((coupling, shares, k * piece, j * width))
    out = None
    for coupling, shares, row_at, column_at in work:
        out = finish(chol, coupling, me * rows, prior, shares, row_at, column_at, out)
    return out


def solution(mesh):
    return jax.shard_map(
        functools.partial(body, mesh.shape["ov"], mesh.shape["vec"]),
        mesh=mesh,
        in_specs=(P("ov", "vec"), P("ov", None), P(("ov", "vec"), None)),
        out_specs=P(("ov", "vec"), None),
        check_vma=False,
    )
```
